256 devices in a mesh: terms: 256 (over z, y, x, core).
Axes of the slice: x: 4, y: 4, z: 8, core: 2. Of those that a mesh axis runs over, the one named last changes fastest.
Arguments:
- psi: float32 [256, 4, 4, 256], replicated
- left_env: bfloat16 [1536, 256, 256], P('terms')
- two_site: bfloat16 [1536, 16, 16], P('terms')
- right_env: bfloat16 [1536, 256, 256], P('terms')
Outputs:
- output 1: float32 [7, 256, 4, 4, 256], replicated
- output 2: float32 [6], replicated
- output 3: float32 [6], replicated
All inputs are finite; a program needn't handle non-finite values.
Results may differ from the reference program's by a relative error of at most 0.0153122.
Values are sent between devices in bfloat16 or wider.
A program may use at most 768 MiB of HBM per device.

```python
import jax
import jax.numpy as jnp
from jax import lax

BOND_DIM = 256
PHYS_DIM = 4
LANCZOS_STEPS = 6
NUM_TERMS = 1536
PAIR_DIM = PHYS_DIM * PHYS_DIM


def sym_draw(key, count, size):
    raw_draw = jax.random.normal(key, (count, size, size), jnp.float32)
    return (raw_draw + jnp.swapaxes(raw_draw, 1, 2)) * (0.5 ** 0.5)


def setup_inputs(seed: int = 0) -> dict:
    keys = jax.random.split(jax.random.key(seed), 4)
    psi = jax.random.normal(keys[0], (BOND_DIM, PHYS_DIM, PHYS_DIM, BOND_DIM), jnp.float32)
    eye_bond = jnp.eye(BOND_DIM, dtype=jnp.float32)
    left_env = eye_bond + sym_draw(keys[1], NUM_TERMS, BOND_DIM) * BOND_DIM ** -0.5
    two_site = sym_draw(keys[2], NUM_TERMS, PAIR_DIM) * (PAIR_DIM * NUM_TERMS) ** -0.5
    right_env = eye_bond + sym_draw(keys[3], NUM_TERMS, BOND_DIM) * BOND_DIM ** -0.5
    return {"psi": psi, "left_env": left_env.astype(jnp.bfloat16), "two_site": two_site.astype(jnp.bfloat16), "right_env": right_env.astype(jnp.bfloat16)}


def apply_ham(vec_bf, left_env, two_site, right_env):
    vec_flat = vec_bf.reshape(BOND_DIM * PAIR_DIM, BOND_DIM)

    def one_term(acc_sum, term):
        left_k, site_k, right_k = term
        right_out = jnp.dot(vec_flat, right_k.T, preferred_element_type=jnp.float32).astype(jnp.bfloat16)
        site_out = jnp.einsum("qp,xpb->xqb", site_k.astype(jnp.float32), right_out.reshape(BOND_DIM, PAIR_DIM, BOND_DIM).astype(jnp.float32)).astype(jnp.bfloat16)
        left_out = jnp.dot(left_k, site_out.reshape(BOND_DIM, PAIR_DIM * BOND_DIM), preferred_element_type=jnp.float32)
        return acc_sum + left_out, None

    init_acc = jnp.zeros((BOND_DIM, PAIR_DIM * BOND_DIM), jnp.float32)
    total = lax.scan(one_term, init_acc, (left_env, two_site, right_env))[0]
    return total.reshape(BOND_DIM, PHYS_DIM, PHYS_DIM, BOND_DIM)


def reference(psi, left_env, two_site, right_env):
    cur_vec = psi / jnp.sqrt(jnp.sum(psi * psi))
    prev_vec = jnp.zeros_like(cur_vec)
    beta_prev = 0.0
    vectors = [cur_vec]
    alphas = []
    betas = []
    for step_idx in range(LANCZOS_STEPS):
        sigma = apply_ham(cur_vec.astype(jnp.bfloat16), left_env, two_site, right_env)
        alpha = jnp.sum(sigma * cur_vec)
        residual = sigma - alpha * cur_vec - beta_prev * prev_vec
        beta = jnp.sqrt(jnp.sum(residual * residual))
        prev_vec = cur_vec
        cur_vec = residual / beta
        vectors.append(cur_vec)
        alphas.append(alpha)
        betas.append(beta)
        beta_prev = beta
    return (jnp.stack(vectors), jnp.stack(alphas), jnp.stack(betas))
```

```python
import jax
import jax.numpy as jnp
from jax import lax
from jax.experimental import pallas as pl
from jax.experimental.pallas import tpu as pltpu
from jax.sharding import PartitionSpec as P

STEPS = 6
D = 256
PAIR = 16
ROWS = PAIR * D
LANES = 128
TERMS = 6
XN, YN, ZN = 4, 4, 8
F32 = jnp.float32
BF16 = jnp.bfloat16
MESH_ID = pl.DeviceIdType.MESH

S1, S2, S3, S4, S5, S6 = range(6)
T1, T2, T3, T4, T5, T6 = range(6, 12)
ZR = 12
ZG = 19
G1, G2, G3, G4 = range(26, 30)
H1, H2, H3, H4 = range(30, 34)
NSEM = 34
CROSS = 5


def rows(start, size):
    return pl.ds(pl.multiple_of(start, 8), size)


def lanczos(psi_hbm, left_hbm, kron_hbm, right_hbm, kry, ab, u, y1a, y1b, y2, part, lbuf, rbuf, wbuf, relay1, final1, relay2, final2, zrecv, load_sem, send_sem, recv_sem, c_send, c_recv, x_send, x_recv):
    me = lax.axis_index("terms")
    core = me % 2
    x = (me // 2) % XN
    y = (me // 8) % YN
    z = me // 32

    def dev(xx, yy, zz, cc):
        return (((zz * YN + yy) * XN + xx) * 2 + cc,)

    xr, xl = dev((x + 1) % XN, y, z, core), dev((x + 3) % XN, y, z, core)
    yr, yl = dev(x, (y + 1) % YN, z, core), dev(x, (y + 3) % YN, z, core)
    zdev = [None] + [dev(x, y, (z + d) % ZN, core) for d in range(1, ZN)]
    other = dev(x, y, z, 1 - core)

    barrier = pltpu.get_barrier_semaphore()
    peers = [xr, xl, yr, yl, other] + zdev[1:]
    for peer in peers:
        pl.semaphore_signal(barrier, inc=1, device_id=peer, device_id_type=MESH_ID)

    loads = []
    for h in range(2):
        for s in range(4):
            for t in range(4):
                loads.append(pltpu.make_async_copy(psi_hbm.at[:, s, t, pl.ds(h * LANES, LANES)], kry.at[0, h, pl.ds((s * 4 + t) * D, D)], load_sem.at[0]))
    for cp in loads:
        cp.start()
    mine = pl.multiple_of(core * TERMS, TERMS)
    own = []
    for k in range(TERMS):
        own.append(pltpu.make_async_copy(left_hbm.at[k], lbuf.at[:, pl.ds(pl.multiple_of((mine + k) * D, D), D)], load_sem.at[1]))
        own.append(pltpu.make_async_copy(right_hbm.at[k, :, pl.ds(pl.multiple_of(core * LANES, LANES), LANES)], rbuf.at[mine + k], load_sem.at[1]))
    own.append(pltpu.make_async_copy(kron_hbm, wbuf.at[pl.ds(mine, TERMS)], load_sem.at[1]))
    for cp in own:
        cp.start()

    pl.semaphore_wait(barrier, len(peers))

    swaps = []
    for k in range(TERMS):
        swaps.append(pltpu.make_async_remote_copy(left_hbm.at[k], lbuf.at[:, pl.ds(pl.multiple_of((mine + k) * D, D), D)], x_send.at[2 * k], x_recv.at[2 * k], device_id=other, device_id_type=MESH_ID))
        swaps.append(pltpu.make_async_remote_copy(right_hbm.at[k, :, pl.ds(pl.multiple_of((1 - core) * LANES, LANES), LANES)], rbuf.at[mine + k], x_send.at[2 * k + 1], x_recv.at[2 * k + 1], device_id=other, device_id_type=MESH_ID))
    swaps.append(pltpu.make_async_remote_copy(kron_hbm, wbuf.at[pl.ds(mine, TERMS)], x_send.at[2 * TERMS], x_recv.at[2 * TERMS], device_id=other, device_id_type=MESH_ID))
    for cp in swaps:
        cp.start()

    CH = 64
    NCH = ROWS // CH

    for cp in loads:
        cp.wait()

    def chunk(i):
        return i // NCH, rows((i % NCH) * CH, CH)

    def sumsq(i, acc):
        h, r = chunk(i)
        val = kry[0, h, r, :]
        return acc + val * val

    zero = jnp.zeros((CH, LANES), F32)

    def total(acc):
        return jnp.broadcast_to(jnp.sum(acc, keepdims=True), (8, LANES))

    norm0 = jnp.sqrt(total(lax.fori_loop(0, 2 * NCH, sumsq, zero)))
    inv0 = jnp.broadcast_to((1.0 / norm0)[:1], (CH, LANES))

    def scale0(i, carry):
        h, r = chunk(i)
        val = kry[0, h, r, :] * inv0
        kry[0, h, r, :] = val
        u[h, r, :] = val.astype(BF16)
        return carry

    lax.fori_loop(0, 2 * NCH, scale0, 0)
    for cp in own:
        cp.wait()
    for cp in swaps:
        cp.wait()

    def right_product(g, out):
        weights = jnp.concatenate([rbuf[2 * g], rbuf[2 * g + 1]], axis=1)
        for m in range(4):
            r = pl.ds(m * 1024, 1024)
            lhs = jnp.concatenate([u[0, r, :], u[1, r, :]], axis=1)
            res = jnp.dot(lhs, weights, preferred_element_type=F32).astype(BF16)
            out[0, r, :] = res[:, :LANES]
            out[1, r, :] = res[:, LANES:]

    def site_product(g, src):
        for t in range(2):
            k = 2 * g + t
            w = wbuf[k]
            for m in range(8):
                cols = []
                for b in range(2):
                    cols.append(jnp.concatenate([src[t, pl.ds(p * D + 32 * m + 16 * b, 16), :] for p in range(PAIR)], axis=0))
                res = jnp.dot(w, jnp.concatenate(cols, axis=1), preferred_element_type=F32).astype(BF16)
                for b in range(2):
                    for q in range(PAIR):
                        y2[q, rows(k * D + 32 * m + 16 * b, 16), :] = res[16 * q : 16 * q + 16, b * LANES : (b + 1) * LANES]

    def left_product(qa, qb):
        rhs = jnp.concatenate([y2[qa], y2[qa + 1], y2[qb], y2[qb + 1]], axis=1)
        res = jnp.dot(lbuf[...], rhs, preferred_element_type=F32)
        for i, q in enumerate((qa, qa + 1, qb, qb + 1)):
            part[rows(q * D, D), :] = res[:, i * LANES : (i + 1) * LANES]

    def step(j, beta_prev):
        nxt = j + 1

        def remote(src, dst, p, s, device):
            return pltpu.make_async_remote_copy(src, dst, send_sem.at[p, s], recv_sem.at[p, s], device_id=device, device_id_type=MESH_ID)

        right_product(0, y1a)

        def two_pairs(i, carry):
            right_product(2 * i + 1, y1b)
            site_product(2 * i, y1a)
            right_product(2 * i + 2, y1a)
            site_product(2 * i + 1, y1b)
            return carry

        lax.fori_loop(0, 2, two_pairs, 0)
        right_product(5, y1b)
        site_product(4, y1a)
        site_product(5, y1b)

        ring1 = [(x, xr, xl, 0), (y, yr, yl, ROWS // 2)]
        ring2 = [(y, yr, yl, 512 * x), (x, xr, xl, ROWS // 2 + 512 * y)]
        sends = []

        def start(cp):
            cp.start()
            sends.append(cp)
            return cp

        def at1(p, d, off, size):
            pos, _, _, base = ring1[p]
            return rows(base + 512 * ((pos + d) % 4) + off, size)

        def at2(p, d, off, size):
            pos, _, _, base = ring2[p]
            return rows(base + 128 * ((pos + d) % 4) + off, size)

        waits = [[None] * 6 for _ in range(2)]
        for d in (2, 1, 3, 0):
            left_product(2 * ((x + d) % 4), 8 + 2 * ((y + d) % 4))
            for p in range(2):
                _, right, left, _ = ring1[p]
                if d == 2:
                    waits[p][0] = start(remote(part.at[at1(p, 2, 0, 256)], relay1.at[p, 0], p, S1, right))
                    waits[p][1] = start(remote(part.at[at1(p, 2, 256, 256)], relay1.at[p, 1], p, S2, left))
                elif d == 1:
                    waits[p][2] = start(remote(part.at[at1(p, 1, 256, 256)], final1.at[p, 0, pl.ds(256, 256)], p, S3, right))
                elif d == 3:
                    waits[p][3] = start(remote(part.at[at1(p, 3, 0, 256)], final1.at[p, 1, pl.ds(0, 256)], p, S4, left))

        def add_into(dst_rows, size, refs):
            for o in range(0, size, 128):
                n = min(128, size - o)
                r = pl.ds(pl.multiple_of(dst_rows.start + o, 8), n)
                acc = part[r, :]
                for ref in refs:
                    acc = acc + ref[pl.ds(o, n), :]
                part[r, :] = acc

        for p in range(2):
            _, right, left, _ = ring1[p]
            waits[p][0].wait_recv()
            add_into(at1(p, 1, 0, 256), 256, [relay1.at[p, 0]])
            waits[p][4] = start(remote(part.at[at1(p, 1, 0, 256)], final1.at[p, 0, pl.ds(0, 256)], p, S5, right))
            waits[p][1].wait_recv()
            add_into(at1(p, 3, 256, 256), 256, [relay1.at[p, 1]])
            waits[p][5] = start(remote(part.at[at1(p, 3, 256, 256)], final1.at[p, 1, pl.ds(256, 256)], p, S6, left))
        for p in range(2):
            for i in (2, 3, 4, 5):
                waits[p][i].wait_recv()
            add_into(at1(p, 0, 0, 512), 512, [final1.at[p, 0], final1.at[p, 1]])

        for p in range(2):
            _, right, left, _ = ring2[p]
            waits[p][0] = start(remote(part.at[at2(p, 2, 0, 64)], relay2.at[p, 0], p, T1, right))
            waits[p][1] = start(remote(part.at[at2(p, 2, 64, 64)], relay2.at[p, 1], p, T2, left))
            waits[p][2] = start(remote(part.at[at2(p, 1, 64, 64)], final2.at[p, 0, pl.ds(64, 64)], p, T3, right))
            waits[p][3] = start(remote(part.at[at2(p, 3, 0, 64)], final2.at[p, 1, pl.ds(0, 64)], p, T4, left))
        for p in range(2):
            _, right, left, _ = ring2[p]
            waits[p][0].wait_recv()
            add_into(at2(p, 1, 0, 64), 64, [relay2.at[p, 0]])
            waits[p][4] = start(remote(part.at[at2(p, 1, 0, 64)], final2.at[p, 0, pl.ds(0, 64)], p, T5, right))
            waits[p][1].wait_recv()
            add_into(at2(p, 3, 64, 64), 64, [relay2.at[p, 1]])
            waits[p][5] = start(remote(part.at[at2(p, 3, 64, 64)], final2.at[p, 1, pl.ds(64, 64)], p, T6, left))
        for p in range(2):
            for i in (2, 3, 4, 5):
                waits[p][i].wait_recv()
            add_into(at2(p, 0, 0, 128), 128, [final2.at[p, 0], final2.at[p, 1]])

        mid = [512 * x + 128 * y, ROWS // 2 + 512 * y + 128 * x]
        zcopies = []
        for d in (4, 3, 5, 2, 6, 1, 7):
            for p in range(2):
                zcopies.append(start(remote(part.at[rows(mid[p] + 16 * ((z + d) % ZN), 16)], zrecv.at[p, d], p, ZR + d - 1, zdev[d])))
        for cp in zcopies:
            cp.wait_recv()
        own_rows = [rows(mid[p] + 16 * z, 16) for p in range(2)]
        for p in range(2):
            acc = part[own_rows[p], :]
            for d in range(1, ZN):
                acc = acc + zrecv[p, d]
            kry[nxt, core, own_rows[p], :] = acc

        zcopies = []
        for d in (4, 3, 5, 2, 6, 1, 7):
            for p in range(2):
                zcopies.append(start(remote(kry.at[nxt, core, own_rows[p]], kry.at[nxt, core, own_rows[p]], p, ZG + d - 1, zdev[d])))
        for cp in zcopies:
            cp.wait_recv()

        def spread(p, src_rows, s, device):
            return start(remote(kry.at[nxt, core, src_rows], kry.at[nxt, core, src_rows], p, s, device))

        g = [[None] * 4 for _ in range(2)]
        for p in range(2):
            _, right, left, _ = ring2[p]
            g[p][0] = spread(p, at2(p, 0, 0, 128), G1, right)
            g[p][1] = spread(p, at2(p, 0, 0, 128), G2, left)
        for p in range(2):
            _, right, left, _ = ring2[p]
            g[p][0].wait_recv()
            g[p][2] = spread(p, at2(p, 3, 0, 64), G3, right)
            g[p][1].wait_recv()
            g[p][3] = spread(p, at2(p, 1, 64, 64), G4, left)
        for p in range(2):
            g[p][2].wait_recv()
            g[p][3].wait_recv()
        h = [[None] * 4 for _ in range(2)]
        crossing = []
        turn = j % 2

        def cross(p, src_rows, i):
            cp = pltpu.make_async_remote_copy(kry.at[nxt, core, src_rows], kry.at[nxt, core, src_rows], c_send.at[turn, p, i], c_recv.at[turn, p, i], device_id=other, device_id_type=MESH_ID)
            crossing.append(start(cp))

        for p in range(2):
            _, right, left, _ = ring1[p]
            h[p][0] = spread(p, at1(p, 0, 0, 512), H1, right)
            h[p][1] = spread(p, at1(p, 0, 0, 512), H2, left)
            cross(p, at1(p, 0, 0, 512), 0)
        for p in range(2):
            _, right, left, _ = ring1[p]
            h[p][0].wait_recv()
            h[p][2] = spread(p, at1(p, 3, 0, 256), H3, right)
            cross(p, at1(p, 3, 0, 512), 1)
            h[p][1].wait_recv()
            h[p][3] = spread(p, at1(p, 1, 256, 256), H4, left)
            cross(p, at1(p, 1, 0, 512), 2)
        for p in range(2):
            h[p][2].wait_recv()
            cross(p, at1(p, 2, 0, 256), 3)
            h[p][3].wait_recv()
            cross(p, at1(p, 2, 256, 256), 4)
        for cp in crossing:
            cp.wait_recv()
        for cp in sends:
            cp.wait_send()

        prev = jnp.maximum(j - 1, 0)

        def dot_chunk(i, acc):
            hh, r = chunk(i)
            return acc + kry[nxt, hh, r, :] * kry[j, hh, r, :]

        alpha = total(lax.fori_loop(0, 2 * NCH, dot_chunk, zero))
        al = jnp.broadcast_to(alpha[:1], (CH, LANES))
        bp = jnp.broadcast_to(beta_prev[:1], (CH, LANES))

        def resid_chunk(i, acc):
            hh, r = chunk(i)
            val = kry[nxt, hh, r, :] - al * kry[j, hh, r, :] - bp * kry[prev, hh, r, :]
            kry[nxt, hh, r, :] = val
            return acc + val * val

        beta = jnp.sqrt(total(lax.fori_loop(0, 2 * NCH, resid_chunk, zero)))
        inv = jnp.broadcast_to((1.0 / beta)[:1], (CH, LANES))

        def scale_chunk(i, carry):
            hh, r = chunk(i)
            val = kry[nxt, hh, r, :] * inv
            kry[nxt, hh, r, :] = val
            u[hh, r, :] = val.astype(BF16)
            return carry

        lax.fori_loop(0, 2 * NCH, scale_chunk, 0)
        ab[0, j] = alpha
        ab[1, j] = beta
        return beta

    lax.fori_loop(0, STEPS, step, jnp.zeros((8, LANES), F32))


def write_out(kry, out, sem):
    copies = []
    for h in range(2):
        for s in range(4):
            for t in range(4):
                copies.append(pltpu.make_async_copy(kry.at[:, h, pl.ds((s * 4 + t) * D, D)], out.at[:, :, s, t, pl.ds(h * LANES, LANES)], sem))
    for cp in copies:
        cp.start()
    for cp in copies:
        cp.wait()


def solution(mesh):
    anywhere = pl.BlockSpec(memory_space=pl.ANY)
    vmem = pl.BlockSpec(memory_space=pltpu.VMEM)

    def body(psi, left_loc, site_loc, right_loc):
        eye = jnp.eye(16, dtype=BF16)
        kron = (site_loc[:, :, None, :, None] * eye[None, None, :, None, :]).reshape(TERMS, D, D)
        kry, ab = pl.pallas_call(
            lanczos,
            out_shape=(pltpu.VMEM((STEPS + 1, 2, ROWS, LANES), F32), pltpu.VMEM((2, STEPS, 8, LANES), F32)),
            in_specs=[anywhere] * 4,
            out_specs=(vmem, vmem),
            scratch_shapes=[
                pltpu.VMEM((2, ROWS, LANES), BF16),
                pltpu.VMEM((2, ROWS, LANES), BF16),
                pltpu.VMEM((2, ROWS, LANES), BF16),
                pltpu.VMEM((PAIR, 2 * TERMS * D, LANES), BF16),
                pltpu.VMEM((ROWS, LANES), F32),
                pltpu.VMEM((D, 2 * TERMS * D), BF16),
                pltpu.VMEM((2 * TERMS, D, LANES), BF16),
                pltpu.VMEM((2 * TERMS, D, D), BF16),
                pltpu.VMEM((2, 2, 256, LANES), F32),
                pltpu.VMEM((2, 2, 512, LANES), F32),
                pltpu.VMEM((2, 2, 64, LANES), F32),
                pltpu.VMEM((2, 2, 128, LANES), F32),
                pltpu.VMEM((2, ZN, 16, LANES), F32),
                pltpu.SemaphoreType.DMA((2,)),
                pltpu.SemaphoreType.DMA((2, NSEM)),
                pltpu.SemaphoreType.DMA((2, NSEM)),
                pltpu.SemaphoreType.DMA((2, 2, CROSS)),
                pltpu.SemaphoreType.DMA((2, 2, CROSS)),
                pltpu.SemaphoreType.DMA((2 * TERMS + 1,)),
                pltpu.SemaphoreType.DMA((2 * TERMS + 1,)),
            ],
            compiler_params=pltpu.CompilerParams(collective_id=0, has_side_effects=True, vmem_limit_bytes=30 * 2**20),
            name="lanczos",
        )(*(pltpu.with_memory_space_constraint(arr, pltpu.HBM) for arr in (psi, left_loc, kron, right_loc)))
        krylov = pl.pallas_call(
            write_out,
            out_shape=jax.ShapeDtypeStruct((STEPS + 1, D, 4, 4, D), F32),
            in_specs=[vmem],
            out_specs=anywhere,
            scratch_shapes=[pltpu.SemaphoreType.DMA],
            compiler_params=pltpu.CompilerParams(vmem_limit_bytes=2**20),
            name="write_out",
        )(pltpu.with_memory_space_constraint(kry, pltpu.VMEM))
        return krylov, ab[0, :, 0, 0], ab[1, :, 0, 0]

    return jax.shard_map(body, mesh=mesh, in_specs=(P(), P("terms"), P("terms"), P("terms")), out_specs=(P(), P(), P()), check_vma=False)
```

```python
import jax
import jax.numpy as jnp
from jax import lax
from jax.experimental import pallas as pl
from jax.experimental.pallas import tpu as pltpu
from jax.sharding import PartitionSpec as P

STEPS = 6
D = 256
PAIR = 16
ROWS = PAIR * D
LANES = 128
TERMS = 6
XN, YN, ZN = 4, 4, 8
F32 = jnp.float32
BF16 = jnp.bfloat16
MESH_ID = pl.DeviceIdType.MESH

S1, S2, S3, S4, S5, S6 = range(6)
T1, T2, T3, T4, T5, T6 = range(6, 12)
ZR = 12
ZG = 19
G1, G2, G3, G4 = range(26, 30)
H0 = 30
NSEM = 46
CROSS = 7
GROUPS = 4


def rows(start, size):
    return pl.ds(pl.multiple_of(start, 8), size)


def lanczos(psi_hbm, left_hbm, site_hbm, right_hbm, kry, ab, u, y1, y2, part, lbuf, rbuf, wraw, wbuf, relay1, final1, relay2, final2, zrecv, load_sem, send_sem, recv_sem, c_send, c_recv, x_send, x_recv):
    me = lax.axis_index("terms")
    core = me % 2
    x = (me // 2) % XN
    y = (me // 8) % YN
    z = me // 32

    def dev(xx, yy, zz, cc):
        return (((zz * YN + yy) * XN + xx) * 2 + cc,)

    xr, xl = dev((x + 1) % XN, y, z, core), dev((x + 3) % XN, y, z, core)
    yr, yl = dev(x, (y + 1) % YN, z, core), dev(x, (y + 3) % YN, z, core)
    zdev = [None] + [dev(x, y, (z + d) % ZN, core) for d in range(1, ZN)]
    other = dev(x, y, z, 1 - core)

    barrier = pltpu.get_barrier_semaphore()
    peers = [xr, xl, yr, yl, other] + zdev[1:]
    for peer in peers:
        pl.semaphore_signal(barrier, inc=1, device_id=peer, device_id_type=MESH_ID)

    loads = []
    for h in range(2):
        for s in range(4):
            for t in range(4):
                loads.append(pltpu.make_async_copy(psi_hbm.at[:, s, t, pl.ds(h * LANES, LANES)], kry.at[0, h, pl.ds((s * 4 + t) * D, D)], load_sem.at[0]))
    for cp in loads:
        cp.start()
    mine = pl.multiple_of(core * TERMS, TERMS)
    own = []
    for k in range(TERMS):
        own.append(pltpu.make_async_copy(left_hbm.at[k], lbuf.at[:, pl.ds(pl.multiple_of((mine + k) * D, D), D)], load_sem.at[1]))
        own.append(pltpu.make_async_copy(right_hbm.at[k, :, pl.ds(pl.multiple_of(core * LANES, LANES), LANES)], rbuf.at[mine + k], load_sem.at[1]))
    own.append(pltpu.make_async_copy(site_hbm, wraw.at[pl.ds(mine, TERMS)], load_sem.at[1]))
    for cp in own:
        cp.start()

    pl.semaphore_wait(barrier, len(peers))

    swaps = []

    def swap(src, dst, i):
        swaps.append(pltpu.make_async_remote_copy(src, dst, x_send.at[i], x_recv.at[i], device_id=other, device_id_type=MESH_ID))

    swap(site_hbm, wraw.at[pl.ds(mine, TERMS)], 2 * TERMS)
    for k in range(TERMS):
        swap(left_hbm.at[k], lbuf.at[:, pl.ds(pl.multiple_of((mine + k) * D, D), D)], 2 * k)
        swap(right_hbm.at[k, :, pl.ds(pl.multiple_of((1 - core) * LANES, LANES), LANES)], rbuf.at[mine + k], 2 * k + 1)
    for cp in swaps:
        cp.start()

    CH = 256
    NCH = ROWS // CH

    for cp in loads:
        cp.wait()

    def chunk(i):
        return i // NCH, rows((i % NCH) * CH, CH)

    def fold(val):
        return jnp.sum(val.reshape(CH // 64, 64, LANES), axis=0)

    zero = jnp.zeros((64, LANES), F32)

    def total(acc):
        return jnp.broadcast_to(jnp.sum(acc, keepdims=True), (8, LANES))

    def wide(val):
        return jnp.broadcast_to(val[:1], (CH, LANES))

    def sumsq(i, acc):
        h, r = chunk(i)
        val = kry[0, h, r, :]
        return acc + fold(val * val)

    norm0 = jnp.sqrt(total(lax.fori_loop(0, 2 * NCH, sumsq, zero)))
    inv0 = wide(1.0 / norm0)

    def scale0(i, carry):
        h, r = chunk(i)
        val = kry[0, h, r, :] * inv0
        kry[0, h, r, :] = val
        u[h, r, :] = val.astype(BF16)
        return carry

    lax.fori_loop(0, 2 * NCH, scale0, 0)
    for cp in own:
        cp.wait()
    for cp in swaps:
        cp.wait()

    spread_rows = (lax.broadcasted_iota(jnp.int32, (D, PAIR), 0) // 16 == lax.broadcasted_iota(jnp.int32, (D, PAIR), 1)).astype(BF16)
    spread_cols = (lax.broadcasted_iota(jnp.int32, (PAIR, D), 1) // 16 == lax.broadcasted_iota(jnp.int32, (PAIR, D), 0)).astype(BF16)
    same = lax.broadcasted_iota(jnp.int32, (D, D), 0) % 16 == lax.broadcasted_iota(jnp.int32, (D, D), 1) % 16

    def build(k, carry):
        tall = jnp.dot(spread_rows, wraw[k], preferred_element_type=F32).astype(BF16)
        full = jnp.dot(tall, spread_cols, preferred_element_type=F32)
        wbuf[k] = jnp.where(same, full, 0.0).astype(BF16)
        return carry

    lax.fori_loop(0, 2 * TERMS, build, 0)

    def right_product(g):
        weights = jnp.concatenate([rbuf[2 * g], rbuf[2 * g + 1]], axis=1)
        for m in range(4):
            r = pl.ds(m * 1024, 1024)
            lhs = jnp.concatenate([u[0, r, :], u[1, r, :]], axis=1)
            res = jnp.dot(lhs, weights, preferred_element_type=F32).astype(BF16)
            y1[2 * g, r, :] = res[:, :LANES]
            y1[2 * g + 1, r, :] = res[:, LANES:]

    def site_product(g, half):
        for t in range(2):
            k = 2 * g + t
            w = wbuf[k, pl.ds(128 * half, 128), :]
            for m in range(8):
                cols = []
                for b in range(2):
                    cols.append(jnp.concatenate([y1[k, pl.ds(p * D + 32 * m + 16 * b, 16), :] for p in range(PAIR)], axis=0))
                res = jnp.dot(w, jnp.concatenate(cols, axis=1), preferred_element_type=F32).astype(BF16)
                for b in range(2):
                    for q in range(8):
                        y2[q, rows(k * D + 32 * m + 16 * b, 16), :] = res[16 * q : 16 * q + 16, b * LANES : (b + 1) * LANES]

    def left_product(half, qs):
        rhs = jnp.concatenate([y2[q] for q in qs], axis=1)
        res = jnp.dot(lbuf[...], rhs, preferred_element_type=F32)
        for i, q in enumerate(qs):
            part[rows((8 * half + q) * D, D), :] = res[:, i * LANES : (i + 1) * LANES]

    ring1 = [(x, xr, xl), (y, yr, yl)] * 2
    ring2 = [(y, yr, yl), (x, xr, xl)] * 2
    ALL = range(GROUPS)
    HALVES = [(0, 1), (2, 3)]

    def chunk_at(n, d):
        return 4 * n * D + D * ((ring1[n][0] + d) % 4)

    def block_at(n, d1, d2):
        return chunk_at(n, d1) + 64 * ((ring2[n][0] + d2) % 4)

    def step(j, beta_prev):
        nxt = j + 1
        turn = j % 2
        sends = []

        def start(src, dst, n, s, device):
            cp = pltpu.make_async_remote_copy(src, dst, send_sem.at[n, s], recv_sem.at[n, s], device_id=device, device_id_type=MESH_ID)
            cp.start()
            sends.append(cp)
            return cp

        def add_into(first, size, refs):
            for o in range(0, size, 128):
                m = min(128, size - o)
                acc = part[rows(first + o, m), :]
                for ref in refs:
                    acc = acc + ref[pl.ds(o, m), :]
                part[rows(first + o, m), :] = acc

        one = [[None] * 6 for _ in ALL]
        two = [[None] * 6 for _ in ALL]

        def scatter1_first(n, d):
            _, right, left = ring1[n]
            first = chunk_at(n, d)
            if d == 2:
                one[n][0] = start(part.at[rows(first, 128)], relay1.at[n, 0], n, S1, right)
                one[n][1] = start(part.at[rows(first + 128, 128)], relay1.at[n, 1], n, S2, left)
            elif d == 1:
                one[n][2] = start(part.at[rows(first + 128, 128)], final1.at[n, 0, pl.ds(128, 128)], n, S3, right)
            elif d == 3:
                one[n][3] = start(part.at[rows(first, 128)], final1.at[n, 1, pl.ds(0, 128)], n, S4, left)

        def scatter1_relay(n):
            _, right, left = ring1[n]
            one[n][0].wait_recv()
            add_into(chunk_at(n, 1), 128, [relay1.at[n, 0]])
            one[n][4] = start(part.at[rows(chunk_at(n, 1), 128)], final1.at[n, 0, pl.ds(0, 128)], n, S5, right)
            one[n][1].wait_recv()
            add_into(chunk_at(n, 3) + 128, 128, [relay1.at[n, 1]])
            one[n][5] = start(part.at[rows(chunk_at(n, 3) + 128, 128)], final1.at[n, 1, pl.ds(128, 128)], n, S6, left)

        def scatter1_final(n):
            for i in (2, 3, 4, 5):
                one[n][i].wait_recv()
            add_into(chunk_at(n, 0), 256, [final1.at[n, 0], final1.at[n, 1]])
            _, right, left = ring2[n]
            two[n][0] = start(part.at[rows(block_at(n, 0, 2), 32)], relay2.at[n, 0], n, T1, right)
            two[n][1] = start(part.at[rows(block_at(n, 0, 2) + 32, 32)], relay2.at[n, 1], n, T2, left)
            two[n][2] = start(part.at[rows(block_at(n, 0, 1) + 32, 32)], final2.at[n, 0, pl.ds(32, 32)], n, T3, right)
            two[n][3] = start(part.at[rows(block_at(n, 0, 3), 32)], final2.at[n, 1, pl.ds(0, 32)], n, T4, left)

        def scatter2_relay(n):
            _, right, left = ring2[n]
            two[n][0].wait_recv()
            add_into(block_at(n, 0, 1), 32, [relay2.at[n, 0]])
            two[n][4] = start(part.at[rows(block_at(n, 0, 1), 32)], final2.at[n, 0, pl.ds(0, 32)], n, T5, right)
            two[n][1].wait_recv()
            add_into(block_at(n, 0, 3) + 32, 32, [relay2.at[n, 1]])
            two[n][5] = start(part.at[rows(block_at(n, 0, 3) + 32, 32)], final2.at[n, 1, pl.ds(32, 32)], n, T6, left)

        far_first = (4, 3, 5, 2, 6, 1, 7)
        zr = [[None] * ZN for _ in ALL]
        zg = [[None] * ZN for _ in ALL]

        def scatter2_final(n):
            for i in (2, 3, 4, 5):
                two[n][i].wait_recv()
            add_into(block_at(n, 0, 0), 64, [final2.at[n, 0], final2.at[n, 1]])

        def scatter_z(group):
            for d in far_first:
                for n in group:
                    zr[n][d] = start(part.at[rows(block_at(n, 0, 0) + 8 * ((z + d) % ZN), 8)], zrecv.at[n, d], n, ZR + d - 1, zdev[d])

        def finish_z(group):
            for n in group:
                r = rows(block_at(n, 0, 0) + 8 * z, 8)
                acc = part[r, :]
                for d in range(1, ZN):
                    zr[n][d].wait_recv()
                    acc = acc + zrecv[n, d]
                kry[nxt, core, r, :] = acc
            for d in far_first:
                for n in group:
                    r = rows(block_at(n, 0, 0) + 8 * z, 8)
                    zg[n][d] = start(kry.at[nxt, core, r], kry.at[nxt, core, r], n, ZG + d - 1, zdev[d])

        def spread(n, first, size, s, device):
            r = rows(first, size)
            return start(kry.at[nxt, core, r], kry.at[nxt, core, r], n, s, device)

        g2 = [[None] * 4 for _ in ALL]
        g1 = [[[None] * 4 for _ in range(4)] for _ in ALL]
        crossing = [[] for _ in ALL]

        def cross(n, first, size):
            r = rows(first, size)
            i = len(crossing[n])
            cp = pltpu.make_async_remote_copy(kry.at[nxt, core, r], kry.at[nxt, core, r], c_send.at[turn, n, i], c_recv.at[turn, n, i], device_id=other, device_id_type=MESH_ID)
            cp.start()
            sends.append(cp)
            crossing[n].append(cp)

        def block_out(n, d2):
            _, right, left = ring1[n]
            g1[n][d2][0] = spread(n, block_at(n, 0, d2), 64, H0 + 4 * d2, right)
            g1[n][d2][1] = spread(n, block_at(n, 0, d2), 64, H0 + 4 * d2 + 1, left)

        def block_on(n, d2):
            _, right, left = ring1[n]
            g1[n][d2][0].wait_recv()
            g1[n][d2][2] = spread(n, block_at(n, 3, d2), 32, H0 + 4 * d2 + 2, right)
            g1[n][d2][1].wait_recv()
            g1[n][d2][3] = spread(n, block_at(n, 1, d2) + 32, 32, H0 + 4 * d2 + 3, left)

        def gather2_first(n):
            for d in range(1, ZN):
                zg[n][d].wait_recv()
            _, right, left = ring2[n]
            g2[n][0] = spread(n, block_at(n, 0, 0), 64, G1, right)
            g2[n][1] = spread(n, block_at(n, 0, 0), 64, G2, left)
            block_out(n, 0)

        def gather2_relay(n):
            _, right, left = ring2[n]
            g2[n][0].wait_recv()
            g2[n][2] = spread(n, block_at(n, 0, 3), 32, G3, right)
            g2[n][1].wait_recv()
            g2[n][3] = spread(n, block_at(n, 0, 1) + 32, 32, G4, left)
            block_out(n, 3)
            block_out(n, 1)

        def gather2_far(n):
            g2[n][2].wait_recv()
            g2[n][3].wait_recv()
            block_out(n, 2)
            cross(n, chunk_at(n, 0), 256)

        def gather1_last(n):
            for d2 in (0, 3, 1, 2):
                g1[n][d2][2].wait_recv()
                g1[n][d2][3].wait_recv()
                cross(n, block_at(n, 2, d2), 64)

        right_product(0)

        def pair_step(g, carry):
            site_product(g, 0)
            right_product(g + 1)
            return carry

        lax.fori_loop(0, TERMS - 1, pair_step, 0)
        site_product(TERMS - 1, 0)

        def site_second(i, carry):
            site_product(2 * i, 1)
            site_product(2 * i + 1, 1)
            return carry

        for half in range(2):
            if half == 1:
                lax.fori_loop(0, TERMS // 2, site_second, 0)
            for ds in ((2, 1), (3, 0)):
                left_product(half, [(x + d) % 4 for d in ds] + [4 + (y + d) % 4 for d in ds])
                for d in ds:
                    for n in HALVES[half]:
                        scatter1_first(n, d)

        def both(*stages):
            for group in HALVES:
                for stage in stages:
                    for n in group:
                        stage(n)

        both(scatter1_relay)
        both(scatter1_final)
        both(scatter2_relay)
        for group in HALVES:
            for n in group:
                scatter2_final(n)
            scatter_z(group)
        for group in HALVES:
            finish_z(group)
        both(gather2_first)
        both(gather2_relay)
        both(gather2_far, lambda n: block_on(n, 0))
        both(lambda n: block_on(n, 3), lambda n: block_on(n, 1))

        def neighbours_done(n):
            block_on(n, 2)
            cross(n, chunk_at(n, 3), 256)
            cross(n, chunk_at(n, 1), 256)

        both(neighbours_done)
        both(gather1_last)

        prev = jnp.maximum(j - 1, 0)
        acc = zero
        for half in range(2):
            for n in HALVES[half]:
                for cp in crossing[n]:
                    cp.wait_recv()

            def dot_chunk(i, total_so_far):
                hh = i // (NCH // 2)
                r = rows(half * (ROWS // 2) + (i % (NCH // 2)) * CH, CH)
                return total_so_far + fold(kry[nxt, hh, r, :] * kry[j, hh, r, :])

            acc = lax.fori_loop(0, NCH, dot_chunk, acc)
        alpha = total(acc)
        al = wide(alpha)
        bp = wide(beta_prev)

        def resid_chunk(i, total_so_far):
            hh, r = chunk(i)
            val = kry[nxt, hh, r, :] - al * kry[j, hh, r, :] - bp * kry[prev, hh, r, :]
            kry[nxt, hh, r, :] = val
            return total_so_far + fold(val * val)

        for cp in sends:
            cp.wait_send()
        beta = jnp.sqrt(total(lax.fori_loop(0, 2 * NCH, resid_chunk, zero)))
        inv = wide(1.0 / beta)

        def scale_chunk(i, carry):
            hh, r = chunk(i)
            val = kry[nxt, hh, r, :] * inv
            kry[nxt, hh, r, :] = val
            u[hh, r, :] = val.astype(BF16)
            return carry

        lax.fori_loop(0, 2 * NCH, scale_chunk, 0)
        ab[0, j] = alpha
        ab[1, j] = beta
        return beta

    lax.fori_loop(0, STEPS, step, jnp.zeros((8, LANES), F32))


def write_out(kry, out, sem):
    copies = []
    for h in range(2):
        for s in range(4):
            for t in range(4):
                copies.append(pltpu.make_async_copy(kry.at[:, h, pl.ds((s * 4 + t) * D, D)], out.at[:, :, s, t, pl.ds(h * LANES, LANES)], sem))
    for cp in copies:
        cp.start()
    for cp in copies:
        cp.wait()


def solution(mesh):
    anywhere = pl.BlockSpec(memory_space=pl.ANY)
    vmem = pl.BlockSpec(memory_space=pltpu.VMEM)

    def body(psi, left_loc, site_loc, right_loc):
        kry, ab = pl.pallas_call(
            lanczos,
            out_shape=(pltpu.VMEM((STEPS + 1, 2, ROWS, LANES), F32), pltpu.VMEM((2, STEPS, 8, LANES), F32)),
            in_specs=[anywhere] * 4,
            out_specs=(vmem, vmem),
            scratch_shapes=[
                pltpu.VMEM((2, ROWS, LANES), BF16),
                pltpu.VMEM((2 * TERMS, ROWS, LANES), BF16),
                pltpu.VMEM((PAIR // 2, 2 * TERMS * D, LANES), BF16),
                pltpu.VMEM((ROWS, LANES), F32),
                pltpu.VMEM((D, 2 * TERMS * D), BF16),
                pltpu.VMEM((2 * TERMS, D, LANES), BF16),
                pltpu.VMEM((2 * TERMS, PAIR, PAIR), BF16),
                pltpu.VMEM((2 * TERMS, D, D), BF16),
                pltpu.VMEM((GROUPS, 2, 128, LANES), F32),
                pltpu.VMEM((GROUPS, 2, 256, LANES), F32),
                pltpu.VMEM((GROUPS, 2, 32, LANES), F32),
                pltpu.VMEM((GROUPS, 2, 64, LANES), F32),
                pltpu.VMEM((GROUPS, ZN, 8, LANES), F32),
                pltpu.SemaphoreType.DMA((2,)),
                pltpu.SemaphoreType.DMA((GROUPS, NSEM)),
                pltpu.SemaphoreType.DMA((GROUPS, NSEM)),
                pltpu.SemaphoreType.DMA((2, GROUPS, CROSS)),
                pltpu.SemaphoreType.DMA((2, GROUPS, CROSS)),
                pltpu.SemaphoreType.DMA((2 * TERMS + 1,)),
                pltpu.SemaphoreType.DMA((2 * TERMS + 1,)),
            ],
            compiler_params=pltpu.CompilerParams(collective_id=0, has_side_effects=True, vmem_limit_bytes=32 * 2**20),
            name="lanczos",
        )(*(pltpu.with_memory_space_constraint(arr, pltpu.HBM) for arr in (psi, left_loc, site_loc, right_loc)))
        krylov = pl.pallas_call(
            write_out,
            out_shape=jax.ShapeDtypeStruct((STEPS + 1, D, 4, 4, D), F32),
            in_specs=[vmem],
            out_specs=anywhere,
            scratch_shapes=[pltpu.SemaphoreType.DMA],
            compiler_params=pltpu.CompilerParams(vmem_limit_bytes=2**20),
            name="write_out",
        )(pltpu.with_memory_space_constraint(kry, pltpu.VMEM))
        return krylov, ab[0, :, 0, 0], ab[1, :, 0, 0]

    return jax.shard_map(body, mesh=mesh, in_specs=(P(), P("terms"), P("terms"), P("terms")), out_specs=(P(), P(), P()), check_vma=False)
```
